32 devices in a mesh: dp: 4 (over x, core), section: 4 (over z), tensor: 2 (over y).
Axes of the slice: x: 2, y: 2, z: 4, core: 2. Of those that a mesh axis runs over, the one named last changes fastest.
Arguments:
- weight_gate: bfloat16 [4096, 11008], P(None, ('dp', 'tensor')), may hold values from -0.09375 to 0.09375
- weight_up: bfloat16 [4096, 11008], P(None, ('dp', 'tensor')), may hold values from -0.09375 to 0.09375
- weight_down: bfloat16 [11008, 4096], P(('dp', 'tensor')), may hold values from -0.0546875 to 0.0546875
- acts_in: bfloat16 [4, 64, 4096], P('section', ('dp', 'tensor')), may hold values from -6 to 6
- grads_in: bfloat16 [4, 64, 4096], P('section', ('dp', 'tensor')), may hold values from -6 to 6
- saved_acts: bfloat16 [4, 4, 64, 4096], P('section', None, ('dp', 'tensor')), may hold values from -6 to 6
- saved_grads: bfloat16 [4, 4, 64, 4096], P('section', None, ('dp', 'tensor')), may hold values from -6 to 6
- plan: int32 [4, 2], P('section'), may hold values from 0 to 3
Outputs:
- next_acts: bfloat16 [4, 64, 4096], P('section', ('dp', 'tensor'))
- next_grads: bfloat16 [4, 64, 4096], P('section', ('dp', 'tensor'))
- grad_gate: bfloat16 [4, 4096, 11008], P('section', None, ('dp', 'tensor'))
- grad_up: bfloat16 [4, 4096, 11008], P('section', None, ('dp', 'tensor'))
The draws below stay inside these ranges and needn't reach their ends.
All inputs are finite; a program needn't handle non-finite values.
Results may differ from the reference program's by a relative error of at most 0.0085.
Values may be sent and summed in bfloat16 or wider, within the bound.
A program may use at most 128 MiB of HBM per device.

```python
import jax
import jax.numpy as jnp
from jax import lax

D = 4096
FF = 11008
TOK = 64
SLOTS = 4
SECTIONS = 4


def plant(entries, key, low, top_value):
    longest = entries.shape.index(max(entries.shape))
    spots = []
    for shift in (0, 1):
        where = [jax.random.randint(jax.random.fold_in(key, axis), (), 0, length) for axis, length in enumerate(entries.shape)]
        where[longest] = (where[longest] + shift) % entries.shape[longest]
        spots.append(tuple(where))
    return entries.at[spots[0]].set(low).at[spots[1]].set(top_value)


def level_of(stream_key, shape, cuts, least, top_value):
    def one(dim, parts):
        steps = jax.random.uniform(jax.random.fold_in(jax.random.fold_in(stream_key, 6), dim), (parts,), jnp.float32, least / len(cuts), top_value / len(cuts))
        return jnp.repeat(jnp.exp(steps), shape[dim] // parts).reshape((-1,) + (1,) * (len(shape) - dim - 1))

    loudness = one(*cuts[0])
    for cut in cuts[1:]:
        loudness = loudness * one(*cut)
    return loudness


def bell_draw(key, shape, deviation, most, shards=(), held_as=jnp.bfloat16):
    loudness = level_of(key, shape, shards, -0.22, 0.18) if shards else 1.0
    entries = jax.random.normal(key, shape, jnp.float32) * deviation * loudness
    return jnp.minimum(jnp.maximum(entries, -most), most).astype(held_as)


def setup_inputs(seed: int = 0) -> dict:
    splits = jax.random.split(jax.random.key(seed), 9)
    weight_gate = bell_draw(splits[0], (D, FF), D ** -0.5, 0.09375, ((1, 8),))
    weight_up = bell_draw(splits[1], (D, FF), D ** -0.5, 0.09375, ((1, 8),))
    weight_down = bell_draw(splits[2], (FF, D), FF ** -0.5, 0.0546875, ((0, 8),))
    acts_in = bell_draw(splits[3], (SECTIONS, TOK, D), 1.0, 6.0, ((0, 4), (1, 8)))
    grads_in = bell_draw(splits[4], (SECTIONS, TOK, D), 1.0, 6.0, ((0, 4), (1, 8)))
    saved_acts = bell_draw(splits[5], (SECTIONS, SLOTS, TOK, D), 1.0, 6.0, ((0, 4), (2, 8)))
    saved_grads = bell_draw(splits[6], (SECTIONS, SLOTS, TOK, D), 1.0, 6.0, ((0, 4), (2, 8)))
    plan = plant(jax.random.randint(splits[7], (SECTIONS, 2), 0, SLOTS), jax.random.fold_in(splits[7], 1), 0, SLOTS - 1).astype(jnp.int32)
    return dict(weight_gate=weight_gate, weight_up=weight_up, weight_down=weight_down, acts_in=acts_in, grads_in=grads_in, saved_acts=saved_acts, saved_grads=saved_grads, plan=plan)


EPS = 0.5

def rms_scale(row_block):
    mean_sq = lax.optimization_barrier(jnp.mean(row_block * row_block, axis=-1, keepdims=True))
    return row_block * lax.rsqrt(mean_sq + EPS)

def gated(normed, w_gate, w_up):
    gate_pre = jnp.dot(normed, w_gate, preferred_element_type=jnp.float32)
    up_pre = jnp.dot(normed, w_up, preferred_element_type=jnp.float32)
    return (gate_pre, up_pre)

def back_gates(cotangent, w_down, gate_pre, up_pre):
    d_act = lax.dot_general(cotangent, w_down, (((1,), (1,)), ((), ())), preferred_element_type=jnp.float32)
    sigmoid_gate = jax.nn.sigmoid(gate_pre)
    d_up = (d_act * gate_pre * sigmoid_gate).astype(jnp.bfloat16)
    d_gate = (d_act * up_pre * sigmoid_gate * (1.0 + gate_pre * (1.0 - sigmoid_gate))).astype(jnp.bfloat16)
    return (d_gate, d_up)

def contract_rows(left, right):
    return lax.dot_general(left, right, (((0,), (0,)), ((), ())), preferred_element_type=jnp.float32)

def reference(weight_gate, weight_up, weight_down, acts_in, grads_in, saved_acts, saved_grads, plan):
    section_count = acts_in.shape[0]
    w_gate = weight_gate
    w_up = weight_up
    w_down = weight_down
    fronts = []
    backs = []
    gate_grads = []
    up_grads = []
    for section_index in range(section_count):
        front_rows = acts_in[section_index]
        back_rows = lax.dynamic_index_in_dim(saved_acts[section_index], plan[section_index, 0], 0, keepdims=False)
        cot_back = grads_in[section_index]
        late_rows = lax.dynamic_index_in_dim(saved_acts[section_index], plan[section_index, 1], 0, keepdims=False)
        cot_late = lax.dynamic_index_in_dim(saved_grads[section_index], plan[section_index, 1], 0, keepdims=False)
        norm_front = rms_scale(front_rows.astype(jnp.float32)).astype(jnp.bfloat16)
        norm_back = rms_scale(back_rows.astype(jnp.float32)).astype(jnp.bfloat16)
        norm_late = rms_scale(late_rows.astype(jnp.float32)).astype(jnp.bfloat16)
        gate_front, up_front = gated(norm_front, w_gate, w_up)
        act_front = (jax.nn.silu(gate_front) * up_front).astype(jnp.bfloat16)
        branch = jnp.dot(act_front, w_down, preferred_element_type=jnp.float32)
        fronts.append((front_rows.astype(jnp.float32) + branch).astype(jnp.bfloat16))
        gate_back, up_back = gated(norm_back, w_gate, w_up)
        dgate_back, dup_back = back_gates(cot_back, w_down, gate_back, up_back)
        d_norm = lax.dot_general(dgate_back, w_gate, (((1,), (1,)), ((), ())), preferred_element_type=jnp.float32)
        d_norm = d_norm + lax.dot_general(dup_back, w_up, (((1,), (1,)), ((), ())), preferred_element_type=jnp.float32)
        unused, norm_pull = jax.vjp(rms_scale, back_rows.astype(jnp.float32))
        d_input = norm_pull(d_norm)[0]
        backs.append((cot_back.astype(jnp.float32) + d_input).astype(jnp.bfloat16))
        gate_late, up_late = gated(norm_late, w_gate, w_up)
        dgate_late, dup_late = back_gates(cot_late, w_down, gate_late, up_late)
        gate_grads.append(contract_rows(norm_late, dgate_late).astype(jnp.bfloat16))
        up_grads.append(contract_rows(norm_late, dup_late).astype(jnp.bfloat16))
    zero_rows = jnp.zeros_like(acts_in[0])
    next_acts = jnp.stack([zero_rows] + fronts[:-1])
    next_grads = jnp.stack(backs[1:] + [zero_rows])
    return (next_acts, next_grads, jnp.stack(gate_grads), jnp.stack(up_grads))
```

```python
import jax
import jax.numpy as jnp
from jax import lax
from jax.experimental import pallas as pl
from jax.experimental.pallas import tpu as pltpu
from jax.sharding import PartitionSpec as P

EPS = 0.5


def shifted(block, axis, distance):
    devices = range(lax.axis_size(axis))
    route = [(i - distance, i) for i in devices if i - distance in devices]
    return lax.ppermute(block, axis, route)


def rms_scale(row_block):
    mean_sq = jnp.mean(row_block * row_block, axis=-1, keepdims=True)
    return row_block * lax.rsqrt(mean_sq + EPS)


def gated(normed, w_gate, w_up):
    gate_pre = jnp.dot(normed, w_gate, preferred_element_type=jnp.float32)
    up_pre = jnp.dot(normed, w_up, preferred_element_type=jnp.float32)
    return (gate_pre, up_pre)


def back_gates(cotangent, w_down, gate_pre, up_pre):
    d_act = lax.dot_general(
        cotangent, w_down, (((1,), (1,)), ((), ())), preferred_element_type=jnp.float32
    )
    sigmoid_gate = jax.nn.sigmoid(gate_pre)
    d_up = (d_act * gate_pre * sigmoid_gate).astype(jnp.bfloat16)
    d_gate = (d_act * up_pre * sigmoid_gate * (1.0 + gate_pre * (1.0 - sigmoid_gate))).astype(
        jnp.bfloat16
    )
    return (d_gate, d_up)


def contract_rows(left, right):
    return lax.dot_general(
        left, right, (((0,), (0,)), ((), ())), preferred_element_type=jnp.float32
    )


def plain_body(weight_gate, weight_up, weight_down, acts_in, grads_in, saved_acts, saved_grads, plan):
    front_rows = acts_in[0]
    cot_back = grads_in[0]
    back_rows = lax.dynamic_index_in_dim(saved_acts[0], plan[0, 0], 0, keepdims=False)
    late_rows = lax.dynamic_index_in_dim(saved_acts[0], plan[0, 1], 0, keepdims=False)
    cot_late = lax.dynamic_index_in_dim(saved_grads[0], plan[0, 1], 0, keepdims=False)
    norm_front = rms_scale(front_rows.astype(jnp.float32)).astype(jnp.bfloat16)
    norm_back = rms_scale(back_rows.astype(jnp.float32)).astype(jnp.bfloat16)
    norm_late = rms_scale(late_rows.astype(jnp.float32)).astype(jnp.bfloat16)
    in_group = (
        lax.all_gather(norm_front, "tensor", axis=0, tiled=True),
        lax.all_gather(norm_back, "tensor", axis=0, tiled=True),
        lax.all_gather(cot_back, "tensor", axis=0, tiled=True),
        lax.all_gather(norm_late, "tensor", axis=0, tiled=True),
        lax.all_gather(cot_late, "tensor", axis=0, tiled=True),
    )
    gathered = (
        lax.all_gather(in_group[0], "dp", axis=0, tiled=True),
        lax.all_gather(in_group[1], "dp", axis=0, tiled=True),
        lax.all_gather(in_group[2], "dp", axis=0, tiled=True),
        lax.all_gather(in_group[3], "dp", axis=0, tiled=True),
        lax.all_gather(in_group[4], "dp", axis=0, tiled=True),
    )
    all_front, all_back, all_cot_back, all_late, all_cot_late = gathered
    gate_front, up_front = gated(all_front, weight_gate, weight_up)
    act_front = (jax.nn.silu(gate_front) * up_front).astype(jnp.bfloat16)
    gate_back, up_back = gated(all_back, weight_gate, weight_up)
    dgate_back, dup_back = back_gates(all_cot_back, weight_down, gate_back, up_back)
    branch = jnp.dot(act_front, weight_down, preferred_element_type=jnp.float32)
    d_norm = lax.dot_general(
        dgate_back, weight_gate, (((1,), (1,)), ((), ())), preferred_element_type=jnp.float32
    )
    d_norm = d_norm + lax.dot_general(
        dup_back, weight_up, (((1,), (1,)), ((), ())), preferred_element_type=jnp.float32
    )
    dp_block = lax.psum_scatter(
        jnp.concatenate([branch, d_norm], axis=1).astype(jnp.bfloat16),
        "dp",
        scatter_dimension=0,
        tiled=True,
    )
    summed = lax.psum_scatter(dp_block, "tensor", scatter_dimension=0, tiled=True).astype(
        jnp.float32
    )
    model_width = front_rows.shape[1]
    branch_rows = summed[:, :model_width]
    d_norm_rows = summed[:, model_width:]
    out_front = (front_rows.astype(jnp.float32) + branch_rows).astype(jnp.bfloat16)
    unused, norm_pull = jax.vjp(rms_scale, back_rows.astype(jnp.float32))
    d_input = norm_pull(d_norm_rows)[0]
    d_rows = (cot_back.astype(jnp.float32) + d_input).astype(jnp.bfloat16)
    next_acts = shifted(out_front, "section", 1)
    next_grads = shifted(d_rows, "section", -1)
    gate_late, up_late = gated(all_late, weight_gate, weight_up)
    dgate_late, dup_late = back_gates(all_cot_late, weight_down, gate_late, up_late)
    grad_gate = contract_rows(all_late, dgate_late).astype(jnp.bfloat16)
    grad_up = contract_rows(all_late, dup_late).astype(jnp.bfloat16)
    return (next_acts[None], next_grads[None], grad_gate[None], grad_up[None])


STEP = 512
NT = (((1,), (1,)), ((), ()))
F32 = jnp.float32
BF16 = jnp.bfloat16
FRONT, BACK, COT_BACK, COT_LATE, LATE = range(5)


def tick_kernel(
    plan, w_gate, w_up, w_down, acts_in, grads_in, saved_acts, saved_grads,
    next_acts, next_grads, late_out, dgate_out, dup_out,
    gate_v, up_v, down_v, blocks, x_fb, x_gh, acc_gate, acc_up, acc_act, act_f, dgate_b, dup_b,
    part, recv_core, held, recv_first, held_next, recv_second, out_rows, in_rows,
    sem_gate, sem_up, sem_down, g_send, g_recv, r_send, r_recv, s_send, s_recv,
):
    dp, y, section = lax.axis_index("dp"), lax.axis_index("tensor"), lax.axis_index("section")
    sections = lax.axis_size("section")
    x, c = dp // 2, dp % 2
    rows, width = acts_in.shape
    steps = width // STEP
    down_cols = width // sem_down.shape[0]
    first_dp = ((1 - x) * (1 - c) + x * c) * 2 + c
    first_y = y * (1 - c) + (1 - y) * c
    second_dp = (x * (1 - c) + (1 - x) * c) * 2 + c
    second_y = (1 - y) * (1 - c) + y * c
    first = {"dp": first_dp, "tensor": first_y}
    second = {"dp": second_dp, "tensor": second_y}
    partner = {"dp": x * 2 + 1 - c}
    after = {"section": (section + 1) % sections}
    before = {"section": (section + sections - 1) % sections}
    own_b = dp * 2 + y
    first_b = first_dp * 2 + first_y
    second_b = second_dp * 2 + second_y
    far_b = ((1 - x) * 2 + c) * 2 + 1 - y
    other = 2 - 4 * c

    def gate_copy(k):
        at = pl.ds(pl.multiple_of(k * STEP, STEP), STEP)
        return pltpu.make_async_copy(w_gate.at[at], gate_v.at[at], sem_gate.at[k])

    def up_copy(k):
        at = pl.ds(pl.multiple_of(k * STEP, STEP), STEP)
        return pltpu.make_async_copy(w_up.at[at], up_v.at[at], sem_up.at[k])

    def down_copy(k):
        at = pl.ds(k * down_cols, down_cols)
        return pltpu.make_async_copy(w_down.at[:, at], down_v.at[:, at], sem_down.at[k])

    def start_weights(k, carry):
        gate_copy(k).start()
        up_copy(k).start()
        return carry

    lax.fori_loop(0, steps, start_weights, 0)
    for k in range(sem_down.shape[0]):
        down_copy(k).start()

    barrier = pltpu.get_barrier_semaphore()
    for peer in (first, second, partner, after, before):
        pl.semaphore_signal(barrier, inc=1, device_id=peer, device_id_type=pl.DeviceIdType.MESH)

    back_slot, late_slot = plan[0, 0], plan[0, 1]
    blocks[FRONT, own_b] = rms_scale(acts_in[...].astype(F32)).astype(BF16)
    blocks[BACK, own_b] = rms_scale(saved_acts[back_slot].astype(F32)).astype(BF16)
    blocks[COT_BACK, own_b] = grads_in[...]
    blocks[COT_LATE, own_b] = saved_grads[late_slot]
    blocks[LATE, own_b] = rms_scale(saved_acts[late_slot].astype(F32)).astype(BF16)
    pl.semaphore_wait(barrier, 5)

    def remote(src, dst, send, recv, peer):
        return pltpu.make_async_remote_copy(
            src_ref=src, dst_ref=dst, send_sem=send, recv_sem=recv,
            device_id=peer, device_id_type=pl.DeviceIdType.MESH,
        )

    def block_copy(a, b, slot, peer):
        return remote(blocks.at[a, b], blocks.at[a, b], g_send.at[a, slot], g_recv.at[a, slot], peer)

    def arrived(a, b, slot):
        block_copy(a, b, slot, partner).wait_recv()

    def send_own(a):
        block_copy(a, own_b, 0, first).start()
        block_copy(a, own_b, 1, second).start()
        block_copy(a, own_b, 3, partner).start()

    def relay(a):
        arrived(a, first_b, 0)
        block_copy(a, first_b, 2, second).start()
        block_copy(a, first_b, 4, partner).start()

    def finish(a):
        arrived(a, second_b, 1)
        block_copy(a, second_b, 5, partner).start()
        arrived(a, far_b, 2)
        block_copy(a, far_b, 6, partner).start()
        for slot, b in ((3, own_b), (4, second_b), (5, first_b), (6, far_b)):
            arrived(a, b + other, slot)

    def assemble(a, out, offset):
        def move(k, carry):
            at = pl.ds(pl.multiple_of(k * STEP, STEP), STEP)
            piece = blocks[a, :, :, at].astype(F32)
            out[offset : offset + piece.shape[0] * rows, at] = piece.reshape(-1, STEP).astype(BF16)
            return carry

        lax.fori_loop(0, steps, move, 0)

    tokens = blocks.shape[1] * rows
    send_own(FRONT)
    send_own(BACK)
    relay(FRONT)
    send_own(COT_BACK)
    relay(BACK)
    send_own(COT_LATE)
    finish(FRONT)
    assemble(FRONT, x_fb, 0)
    finish(BACK)
    assemble(BACK, x_fb, tokens)

    def up_front(k, carry):
        gate_copy(k).wait()
        up_copy(k).wait()
        at = pl.ds(pl.multiple_of(k * STEP, STEP), STEP)
        piece = x_fb[:, at]
        acc_gate[...] += jnp.dot(piece, gate_v[at, :], preferred_element_type=F32)
        acc_up[...] += jnp.dot(piece, up_v[at, :], preferred_element_type=F32)
        return carry

    acc_gate[...] = jnp.zeros_like(acc_gate)
    acc_up[...] = jnp.zeros_like(acc_up)
    lax.fori_loop(0, steps // 2, up_front, 0)
    relay(COT_BACK)
    send_own(LATE)
    relay(COT_LATE)
    lax.fori_loop(steps // 2, steps, up_front, 0)
    finish(COT_BACK)
    assemble(COT_BACK, x_gh, 0)
    relay(LATE)
    finish(COT_LATE)
    assemble(COT_LATE, x_gh, tokens)

    for k in range(sem_down.shape[0]):
        down_copy(k).wait()

    def d_act_step(k, carry):
        at = pl.ds(pl.multiple_of(k * STEP, STEP), STEP)
        acc_act[...] += lax.dot_general(x_gh[:, at], down_v[:, at], NT, preferred_element_type=F32)
        return carry

    acc_act[...] = jnp.zeros_like(acc_act)
    lax.fori_loop(0, steps, d_act_step, 0)

    def back_of(d_act, gate_pre, up_pre):
        sigmoid_gate = jax.nn.sigmoid(gate_pre)
        d_up = (d_act * gate_pre * sigmoid_gate).astype(BF16)
        d_gate = (d_act * up_pre * sigmoid_gate * (1.0 + gate_pre * (1.0 - sigmoid_gate))).astype(BF16)
        return d_gate, d_up

    group = 16

    def pointwise(i, carry):
        at = pl.ds(pl.multiple_of(i * group, group), group)
        low = pl.ds(pl.multiple_of(tokens + i * group, group), group)
        dgate_b[at, :], dup_b[at, :] = back_of(acc_act[at, :], acc_gate[low, :], acc_up[low, :])
        gate_pre = acc_gate[at, :]
        act_f[at, :] = (gate_pre * jax.nn.sigmoid(gate_pre) * acc_up[at, :]).astype(BF16)
        return carry

    lax.fori_loop(0, tokens // group, pointwise, 0)

    def put_part(r, at, total):
        for b in range(8):
            part[r, (b // 2) % 2, b // 4, b % 2, :, at] = total[b * rows : (b + 1) * rows].astype(BF16)

    def d_norm_step(k, carry):
        at = pl.ds(pl.multiple_of(k * STEP, STEP), STEP)
        total = lax.dot_general(dgate_b[...], gate_v[at, :], NT, preferred_element_type=F32)
        total += lax.dot_general(dup_b[...], up_v[at, :], NT, preferred_element_type=F32)
        put_part(0, at, total)
        return carry

    def branch_step(k, carry):
        at = pl.ds(pl.multiple_of(k * STEP, STEP), STEP)
        put_part(1, at, jnp.dot(act_f[...], down_v[:, at], preferred_element_type=F32))
        return carry

    mine_first = x * (1 - c) + y * c
    mine_second = y * (1 - c) + x * c

    def core_copy(r):
        return remote(part.at[r, 1 - c], recv_core.at[r], r_send.at[r, 0], r_recv.at[r, 0], partner)

    def first_copy(r):
        return remote(held.at[r, 1 - mine_first], recv_first.at[r], r_send.at[r, 1], r_recv.at[r, 1], first)

    def second_copy(r):
        return remote(held_next.at[r, 1 - mine_second], recv_second.at[r], r_send.at[r, 2], r_recv.at[r, 2], second)

    def add_core(r):
        core_copy(r).wait_recv()
        for f in range(2):
            for s in range(2):
                at_x = f * (1 - c) + s * c
                at_y = s * (1 - c) + f * c
                mine = part[r, c, at_x, at_y].astype(F32)
                held[r, f, s] = (mine + recv_core[r, at_x, at_y].astype(F32)).astype(BF16)
        first_copy(r).start()

    def add_first(r):
        first_copy(r).wait_recv()
        for s in range(2):
            mine = held[r, mine_first, s].astype(F32)
            held_next[r, s] = (mine + recv_first[r, s].astype(F32)).astype(BF16)
        second_copy(r).start()

    def add_second(r):
        second_copy(r).wait_recv()
        return held_next[r, mine_second].astype(F32) + recv_second[r].astype(F32)

    def shift(r):
        return remote(out_rows.at[r], in_rows.at[r], s_send.at[r], s_recv.at[r], before if r == 0 else after)

    lax.fori_loop(0, steps, d_norm_step, 0)
    core_copy(0).start()
    lax.fori_loop(0, steps, branch_step, 0)
    core_copy(1).start()
    add_core(0)
    finish(LATE)
    assemble(LATE, late_out, 0)

    def up_late(k, carry):
        at = pl.ds(pl.multiple_of(k * STEP, STEP), STEP)
        piece = late_out[:, at]
        acc_gate[:tokens] += jnp.dot(piece, gate_v[at, :], preferred_element_type=F32)
        acc_up[:tokens] += jnp.dot(piece, up_v[at, :], preferred_element_type=F32)
        return carry

    acc_gate[:tokens] = jnp.zeros((tokens, acc_gate.shape[1]), F32)
    acc_up[:tokens] = jnp.zeros((tokens, acc_up.shape[1]), F32)
    add_core(1)
    lax.fori_loop(0, steps // 2, up_late, 0)
    add_first(0)
    add_first(1)
    lax.fori_loop(steps // 2, steps, up_late, 0)

    d_norm = add_second(0)
    rows_b = saved_acts[back_slot].astype(F32)
    scale = lax.rsqrt(jnp.mean(rows_b * rows_b, axis=-1, keepdims=True) + EPS)
    along = jnp.mean(d_norm * rows_b, axis=-1, keepdims=True)
    d_input = d_norm * scale - rows_b * (scale * scale * scale * along)
    out_rows[0] = (grads_in[...].astype(F32) + d_input).astype(BF16)

    @pl.when(section > 0)
    def _():
        shift(0).start()

    out_rows[1] = (acts_in[...].astype(F32) + add_second(1)).astype(BF16)

    @pl.when(section < sections - 1)
    def _():
        shift(1).start()

    def pointwise_late(i, carry):
        at = pl.ds(pl.multiple_of(i * group, group), group)
        low = pl.ds(pl.multiple_of(tokens + i * group, group), group)
        dgate_out[at, :], dup_out[at, :] = back_of(acc_act[low, :], acc_gate[at, :], acc_up[at, :])
        return carry

    lax.fori_loop(0, tokens // group, pointwise_late, 0)

    @pl.when(section < sections - 1)
    def _():
        shift(0).wait_recv()
        next_grads[...] = in_rows[0]

    @pl.when(section == sections - 1)
    def _():
        next_grads[...] = jnp.zeros_like(next_grads)

    @pl.when(section > 0)
    def _():
        shift(1).wait_recv()
        next_acts[...] = in_rows[1]
        shift(0).wait_send()

    @pl.when(section == 0)
    def _():
        next_acts[...] = jnp.zeros_like(next_acts)

    @pl.when(section < sections - 1)
    def _():
        shift(1).wait_send()

    for r in range(2):
        core_copy(r).wait_send()
        first_copy(r).wait_send()
        second_copy(r).wait_send()
    for a in range(5):
        for slot in range(7):
            block_copy(a, own_b, slot, partner).wait_send()


def outer_kernel(late, d_gate, d_up, grad_gate, grad_up):
    left = late[...]
    grad_gate[...] = contract_rows(left, d_gate[...]).astype(BF16)
    grad_up[...] = contract_rows(left, d_up[...]).astype(BF16)


def outer(late, d_gate, d_up):
    tokens, width = late.shape
    hidden = d_gate.shape[1]
    whole = pl.BlockSpec((tokens, hidden), lambda i: (0, 0))
    tile = pl.BlockSpec((STEP, hidden), lambda i: (i, 0))
    return pl.pallas_call(
        outer_kernel,
        grid=(width // STEP,),
        out_shape=(jax.ShapeDtypeStruct((width, hidden), BF16),) * 2,
        in_specs=[pl.BlockSpec((tokens, STEP), lambda i: (0, i)), whole, whole],
        out_specs=(tile, tile),
        cost_estimate=pl.CostEstimate(
            flops=4 * tokens * width * hidden, bytes_accessed=4 * width * hidden, transcendentals=0
        ),
    )(late, d_gate, d_up)


def body(weight_gate, weight_up, weight_down, acts_in, grads_in, saved_acts, saved_grads, plan):
    width, hidden = weight_gate.shape
    rows = acts_in.shape[1]
    blocks = 8
    tokens = rows * blocks
    vmem = pl.BlockSpec(memory_space=pltpu.VMEM)
    hbm = pl.BlockSpec(memory_space=pl.ANY)
    dma = pltpu.SemaphoreType.DMA
    small = jax.ShapeDtypeStruct((rows, width), BF16)
    narrow = jax.ShapeDtypeStruct((tokens, hidden), BF16)
    next_acts, next_grads, late, d_gate, d_up = pl.pallas_call(
        tick_kernel,
        out_shape=(small, small, jax.ShapeDtypeStruct((tokens, width), BF16), narrow, narrow),
        in_specs=[pl.BlockSpec(memory_space=pltpu.SMEM), hbm, hbm, hbm, vmem, vmem, vmem, vmem],
        out_specs=(vmem,) * 5,
        scratch_shapes=[
            pltpu.VMEM((width, hidden), BF16),
            pltpu.VMEM((width, hidden), BF16),
            pltpu.VMEM((hidden, width), BF16),
            pltpu.VMEM((5, blocks, rows, width), BF16),
            pltpu.VMEM((2 * tokens, width), BF16),
            pltpu.VMEM((2 * tokens, width), BF16),
            pltpu.VMEM((2 * tokens, hidden), F32),
            pltpu.VMEM((2 * tokens, hidden), F32),
            pltpu.VMEM((2 * tokens, hidden), F32),
            pltpu.VMEM((tokens, hidden), BF16),
            pltpu.VMEM((tokens, hidden), BF16),
            pltpu.VMEM((tokens, hidden), BF16),
            pltpu.VMEM((2, 2, 2, 2, rows, width), BF16),
            pltpu.VMEM((2, 2, 2, rows, width), BF16),
            pltpu.VMEM((2, 2, 2, rows, width), BF16),
            pltpu.VMEM((2, 2, rows, width), BF16),
            pltpu.VMEM((2, 2, rows, width), BF16),
            pltpu.VMEM((2, rows, width), BF16),
            pltpu.VMEM((2, rows, width), BF16),
            pltpu.VMEM((2, rows, width), BF16),
            dma((width // STEP,)),
            dma((width // STEP,)),
            dma((4,)),
            dma((5, 7)),
            dma((5, 7)),
            dma((2, 3)),
            dma((2, 3)),
            dma((2,)),
            dma((2,)),
        ],
        compiler_params=pltpu.CompilerParams(
            collective_id=0, has_side_effects=True, vmem_limit_bytes=64 * 1024 * 1000
        ),
    )(
        plan, weight_gate, weight_up, weight_down,
        acts_in[0], grads_in[0], saved_acts[0], saved_grads[0],
    )
    grad_gate, grad_up = outer(late, d_gate, d_up)
    return (next_acts[None], next_grads[None], grad_gate[None], grad_up[None])


def solution(mesh):
    placed = (
        P(None, ("dp", "tensor")),
        P(None, ("dp", "tensor")),
        P(("dp", "tensor"), None),
        P("section", ("dp", "tensor"), None),
        P("section", ("dp", "tensor"), None),
        P("section", None, ("dp", "tensor"), None),
        P("section", None, ("dp", "tensor"), None),
        P("section", None),
    )

    def chosen(*arrays):
        width = arrays[0].shape[0]
        rows = arrays[3].shape[1]
        square = mesh.shape["dp"] == 4 and mesh.shape["tensor"] == 2
        fits = square and rows % 8 == 0 and width % (2 * STEP) == 0 and arrays[0].shape[1] % 16 == 0
        return (body if fits else plain_body)(*arrays)

    return jax.shard_map(
        chosen,
        mesh=mesh,
        in_specs=placed,
        out_specs=(
            P("section", ("dp", "tensor"), None),
            P("section", ("dp", "tensor"), None),
            P("section", None, ("dp", "tensor")),
            P("section", None, ("dp", "tensor")),
        ),
        check_vma=False,
    )
```

```python
import jax
import jax.numpy as jnp
from jax import lax
from jax.experimental import pallas as pl
from jax.experimental.pallas import tpu as pltpu
from jax.sharding import PartitionSpec as P

EPS = 0.5


def shifted(block, axis, distance):
    devices = range(lax.axis_size(axis))
    route = [(i - distance, i) for i in devices if i - distance in devices]
    return lax.ppermute(block, axis, route)


def rms_scale(row_block):
    mean_sq = jnp.mean(row_block * row_block, axis=-1, keepdims=True)
    return row_block * lax.rsqrt(mean_sq + EPS)


def gated(normed, w_gate, w_up):
    gate_pre = jnp.dot(normed, w_gate, preferred_element_type=jnp.float32)
    up_pre = jnp.dot(normed, w_up, preferred_element_type=jnp.float32)
    return (gate_pre, up_pre)


def back_gates(cotangent, w_down, gate_pre, up_pre):
    d_act = lax.dot_general(
        cotangent, w_down, (((1,), (1,)), ((), ())), preferred_element_type=jnp.float32
    )
    sigmoid_gate = jax.nn.sigmoid(gate_pre)
    d_up = (d_act * gate_pre * sigmoid_gate).astype(jnp.bfloat16)
    d_gate = (d_act * up_pre * sigmoid_gate * (1.0 + gate_pre * (1.0 - sigmoid_gate))).astype(
        jnp.bfloat16
    )
    return (d_gate, d_up)


def contract_rows(left, right):
    return lax.dot_general(
        left, right, (((0,), (0,)), ((), ())), preferred_element_type=jnp.float32
    )


def plain_body(weight_gate, weight_up, weight_down, acts_in, grads_in, saved_acts, saved_grads, plan):
    front_rows = acts_in[0]
    cot_back = grads_in[0]
    back_rows = lax.dynamic_index_in_dim(saved_acts[0], plan[0, 0], 0, keepdims=False)
    late_rows = lax.dynamic_index_in_dim(saved_acts[0], plan[0, 1], 0, keepdims=False)
    cot_late = lax.dynamic_index_in_dim(saved_grads[0], plan[0, 1], 0, keepdims=False)
    norm_front = rms_scale(front_rows.astype(jnp.float32)).astype(jnp.bfloat16)
    norm_back = rms_scale(back_rows.astype(jnp.float32)).astype(jnp.bfloat16)
    norm_late = rms_scale(late_rows.astype(jnp.float32)).astype(jnp.bfloat16)
    in_group = (
        lax.all_gather(norm_front, "tensor", axis=0, tiled=True),
        lax.all_gather(norm_back, "tensor", axis=0, tiled=True),
        lax.all_gather(cot_back, "tensor", axis=0, tiled=True),
        lax.all_gather(norm_late, "tensor", axis=0, tiled=True),
        lax.all_gather(cot_late, "tensor", axis=0, tiled=True),
    )
    gathered = (
        lax.all_gather(in_group[0], "dp", axis=0, tiled=True),
        lax.all_gather(in_group[1], "dp", axis=0, tiled=True),
        lax.all_gather(in_group[2], "dp", axis=0, tiled=True),
        lax.all_gather(in_group[3], "dp", axis=0, tiled=True),
        lax.all_gather(in_group[4], "dp", axis=0, tiled=True),
    )
    all_front, all_back, all_cot_back, all_late, all_cot_late = gathered
    gate_front, up_front = gated(all_front, weight_gate, weight_up)
    act_front = (jax.nn.silu(gate_front) * up_front).astype(jnp.bfloat16)
    gate_back, up_back = gated(all_back, weight_gate, weight_up)
    dgate_back, dup_back = back_gates(all_cot_back, weight_down, gate_back, up_back)
    branch = jnp.dot(act_front, weight_down, preferred_element_type=jnp.float32)
    d_norm = lax.dot_general(
        dgate_back, weight_gate, (((1,), (1,)), ((), ())), preferred_element_type=jnp.float32
    )
    d_norm = d_norm + lax.dot_general(
        dup_back, weight_up, (((1,), (1,)), ((), ())), preferred_element_type=jnp.float32
    )
    dp_block = lax.psum_scatter(
        jnp.concatenate([branch, d_norm], axis=1).astype(jnp.bfloat16),
        "dp",
        scatter_dimension=0,
        tiled=True,
    )
    summed = lax.psum_scatter(dp_block, "tensor", scatter_dimension=0, tiled=True).astype(
        jnp.float32
    )
    model_width = front_rows.shape[1]
    branch_rows = summed[:, :model_width]
    d_norm_rows = summed[:, model_width:]
    out_front = (front_rows.astype(jnp.float32) + branch_rows).astype(jnp.bfloat16)
    unused, norm_pull = jax.vjp(rms_scale, back_rows.astype(jnp.float32))
    d_input = norm_pull(d_norm_rows)[0]
    d_rows = (cot_back.astype(jnp.float32) + d_input).astype(jnp.bfloat16)
    next_acts = shifted(out_front, "section", 1)
    next_grads = shifted(d_rows, "section", -1)
    gate_late, up_late = gated(all_late, weight_gate, weight_up)
    dgate_late, dup_late = back_gates(all_cot_late, weight_down, gate_late, up_late)
    grad_gate = contract_rows(all_late, dgate_late).astype(jnp.bfloat16)
    grad_up = contract_rows(all_late, dup_late).astype(jnp.bfloat16)
    return (next_acts[None], next_grads[None], grad_gate[None], grad_up[None])


STEP = 512
NT = (((1,), (1,)), ((), ()))
F32 = jnp.float32
BF16 = jnp.bfloat16
FRONT, BACK, COT_BACK, COT_LATE, LATE = range(5)


def tick_kernel(
    plan, w_gate, w_up, w_down, acts_in, grads_in, saved_acts, saved_grads,
    next_acts, next_grads, late_out, dgate_out, dup_out,
    gate_v, up_v, down_v, blocks, x_fb, x_gh, acc_gate, acc_up, acc_act, act_f, dgate_b, dup_b,
    part, recv_core, held, recv_first, held_next, recv_second, out_rows, in_rows,
    sem_gate, sem_up, sem_down, g_send, g_recv, r_send, r_recv, s_send, s_recv,
):
    dp, y, section = lax.axis_index("dp"), lax.axis_index("tensor"), lax.axis_index("section")
    sections = lax.axis_size("section")
    x, c = dp // 2, dp % 2
    rows, width = acts_in.shape
    steps = width // STEP
    down_cols = width // sem_down.shape[0]
    first_dp = ((1 - x) * (1 - c) + x * c) * 2 + c
    first_y = y * (1 - c) + (1 - y) * c
    second_dp = (x * (1 - c) + (1 - x) * c) * 2 + c
    second_y = (1 - y) * (1 - c) + y * c
    first = {"dp": first_dp, "tensor": first_y}
    second = {"dp": second_dp, "tensor": second_y}
    partner = {"dp": x * 2 + 1 - c}
    after = {"section": (section + 1) % sections}
    before = {"section": (section + sections - 1) % sections}
    own_b = dp * 2 + y
    first_b = first_dp * 2 + first_y
    second_b = second_dp * 2 + second_y
    far_b = ((1 - x) * 2 + c) * 2 + 1 - y
    other = 2 - 4 * c

    def gate_copy(k):
        at = pl.ds(pl.multiple_of(k * STEP, STEP), STEP)
        return pltpu.make_async_copy(w_gate.at[:, at], gate_v.at[:, at], sem_gate.at[k])

    def up_copy(k):
        at = pl.ds(pl.multiple_of(k * STEP, STEP), STEP)
        return pltpu.make_async_copy(w_up.at[:, at], up_v.at[:, at], sem_up.at[k])

    def down_copy(k):
        at = pl.ds(k * down_cols, down_cols)
        return pltpu.make_async_copy(w_down.at[:, at], down_v.at[:, at], sem_down.at[k])

    def start_weights(k, carry):
        gate_copy(k).start()
        up_copy(k).start()
        return carry

    lax.fori_loop(0, steps, start_weights, 0)
    for k in range(sem_down.shape[0]):
        down_copy(k).start()

    barrier = pltpu.get_barrier_semaphore()
    for peer in (first, second, partner, after, before):
        pl.semaphore_signal(barrier, inc=1, device_id=peer, device_id_type=pl.DeviceIdType.MESH)

    back_slot, late_slot = plan[0, 0], plan[0, 1]
    blocks[FRONT, own_b] = rms_scale(acts_in[...].astype(F32)).astype(BF16)
    blocks[BACK, own_b] = rms_scale(saved_acts[back_slot].astype(F32)).astype(BF16)
    blocks[COT_BACK, own_b] = grads_in[...]
    blocks[COT_LATE, own_b] = saved_grads[late_slot]
    blocks[LATE, own_b] = rms_scale(saved_acts[late_slot].astype(F32)).astype(BF16)
    pl.semaphore_wait(barrier, 5)

    def remote(src, dst, send, recv, peer):
        return pltpu.make_async_remote_copy(
            src_ref=src, dst_ref=dst, send_sem=send, recv_sem=recv,
            device_id=peer, device_id_type=pl.DeviceIdType.MESH,
        )

    def block_copy(a, b, slot, peer):
        return remote(blocks.at[a, b], blocks.at[a, b], g_send.at[a, slot], g_recv.at[a, slot], peer)

    def arrived(a, b, slot):
        block_copy(a, b, slot, partner).wait_recv()

    def send_own(a):
        block_copy(a, own_b, 0, first).start()
        block_copy(a, own_b, 1, second).start()
        block_copy(a, own_b, 3, partner).start()

    def relay(a):
        arrived(a, first_b, 0)
        block_copy(a, first_b, 2, second).start()
        block_copy(a, first_b, 4, partner).start()

    def finish(a):
        arrived(a, second_b, 1)
        block_copy(a, second_b, 5, partner).start()
        arrived(a, far_b, 2)
        block_copy(a, far_b, 6, partner).start()
        for slot, b in ((3, own_b), (4, second_b), (5, first_b), (6, far_b)):
            arrived(a, b + other, slot)

    def assemble(a, out, offset):
        def move(k, carry):
            at = pl.ds(pl.multiple_of(k * STEP, STEP), STEP)
            piece = blocks[a, :, :, at].astype(F32)
            out[offset : offset + piece.shape[0] * rows, at] = piece.reshape(-1, STEP).astype(BF16)
            return carry

        lax.fori_loop(0, steps, move, 0)

    tokens = blocks.shape[1] * rows
    send_own(FRONT)
    send_own(BACK)
    relay(FRONT)
    send_own(COT_BACK)
    relay(BACK)
    send_own(COT_LATE)
    finish(FRONT)
    assemble(FRONT, x_fb, 0)
    finish(BACK)
    assemble(BACK, x_fb, tokens)

    def up_front(k, carry):
        gate_copy(k).wait()
        up_copy(k).wait()
        at = pl.ds(pl.multiple_of(k * STEP, STEP), STEP)
        piece = x_fb[:, at]
        acc_gate[...] += lax.dot_general(piece, gate_v[:, at], NT, preferred_element_type=F32)
        acc_up[...] += lax.dot_general(piece, up_v[:, at], NT, preferred_element_type=F32)
        return carry

    acc_gate[...] = jnp.zeros_like(acc_gate)
    acc_up[...] = jnp.zeros_like(acc_up)
    lax.fori_loop(0, steps // 2, up_front, 0)
    relay(COT_BACK)
    send_own(LATE)
    relay(COT_LATE)
    lax.fori_loop(steps // 2, steps, up_front, 0)
    finish(COT_BACK)
    assemble(COT_BACK, x_gh, 0)
    relay(LATE)
    finish(COT_LATE)
    assemble(COT_LATE, x_gh, tokens)

    for k in range(sem_down.shape[0]):
        down_copy(k).wait()

    def d_act_step(k, carry):
        at = pl.ds(pl.multiple_of(k * STEP, STEP), STEP)
        acc_act[...] += lax.dot_general(x_gh[:, at], down_v[:, at], NT, preferred_element_type=F32)
        return carry

    acc_act[...] = jnp.zeros_like(acc_act)
    lax.fori_loop(0, steps, d_act_step, 0)

    def back_of(d_act, gate_pre, up_pre):
        sigmoid_gate = jax.nn.sigmoid(gate_pre)
        d_up = (d_act * gate_pre * sigmoid_gate).astype(BF16)
        d_gate = (d_act * up_pre * sigmoid_gate * (1.0 + gate_pre * (1.0 - sigmoid_gate))).astype(BF16)
        return d_gate, d_up

    group = 16

    def pointwise(i, carry):
        at = pl.ds(pl.multiple_of(i * group, group), group)
        low = pl.ds(pl.multiple_of(tokens + i * group, group), group)
        dgate_b[at, :], dup_b[at, :] = back_of(acc_act[at, :], acc_gate[low, :], acc_up[low, :])
        gate_pre = acc_gate[at, :]
        act_f[at, :] = (gate_pre * jax.nn.sigmoid(gate_pre) * acc_up[at, :]).astype(BF16)
        return carry

    lax.fori_loop(0, tokens // group, pointwise, 0)

    def put_part(r, at, total):
        for b in range(8):
            part[r, (b // 2) % 2, b // 4, b % 2, :, at] = total[b * rows : (b + 1) * rows].astype(BF16)

    def d_norm_step(k, carry):
        at = pl.ds(pl.multiple_of(k * STEP, STEP), STEP)
        total = jnp.dot(dgate_b[...], gate_v[:, at], preferred_element_type=F32)
        total += jnp.dot(dup_b[...], up_v[:, at], preferred_element_type=F32)
        put_part(0, at, total)
        return carry

    def branch_step(k, carry):
        at = pl.ds(pl.multiple_of(k * STEP, STEP), STEP)
        put_part(1, at, jnp.dot(act_f[...], down_v[:, at], preferred_element_type=F32))
        return carry

    mine_first = x * (1 - c) + y * c
    mine_second = y * (1 - c) + x * c

    def core_copy(r):
        return remote(part.at[r, 1 - c], recv_core.at[r], r_send.at[r, 0], r_recv.at[r, 0], partner)

    def first_copy(r):
        return remote(held.at[r, 1 - mine_first], recv_first.at[r], r_send.at[r, 1], r_recv.at[r, 1], first)

    def second_copy(r):
        return remote(held_next.at[r, 1 - mine_second], recv_second.at[r], r_send.at[r, 2], r_recv.at[r, 2], second)

    def add_core(r):
        core_copy(r).wait_recv()
        for f in range(2):
            for s in range(2):
                at_x = f * (1 - c) + s * c
                at_y = s * (1 - c) + f * c
                mine = part[r, c, at_x, at_y].astype(F32)
                held[r, f, s] = (mine + recv_core[r, at_x, at_y].astype(F32)).astype(BF16)
        first_copy(r).start()

    def add_first(r):
        first_copy(r).wait_recv()
        for s in range(2):
            mine = held[r, mine_first, s].astype(F32)
            held_next[r, s] = (mine + recv_first[r, s].astype(F32)).astype(BF16)
        second_copy(r).start()

    def add_second(r):
        second_copy(r).wait_recv()
        return held_next[r, mine_second].astype(F32) + recv_second[r].astype(F32)

    def shift(r):
        return remote(out_rows.at[r], in_rows.at[r], s_send.at[r], s_recv.at[r], before if r == 0 else after)

    lax.fori_loop(0, steps, d_norm_step, 0)
    core_copy(0).start()
    lax.fori_loop(0, steps, branch_step, 0)
    core_copy(1).start()
    add_core(0)
    finish(LATE)
    assemble(LATE, late_out, 0)

    def up_late(k, carry):
        at = pl.ds(pl.multiple_of(k * STEP, STEP), STEP)
        piece = late_out[:, at]
        acc_gate[:tokens] += lax.dot_general(piece, gate_v[:, at], NT, preferred_element_type=F32)
        acc_up[:tokens] += lax.dot_general(piece, up_v[:, at], NT, preferred_element_type=F32)
        return carry

    acc_gate[:tokens] = jnp.zeros((tokens, acc_gate.shape[1]), F32)
    acc_up[:tokens] = jnp.zeros((tokens, acc_up.shape[1]), F32)
    add_core(1)
    lax.fori_loop(0, steps // 2, up_late, 0)
    add_first(0)
    add_first(1)
    lax.fori_loop(steps // 2, steps, up_late, 0)

    d_norm = add_second(0)
    rows_b = saved_acts[back_slot].astype(F32)
    scale = lax.rsqrt(jnp.mean(rows_b * rows_b, axis=-1, keepdims=True) + EPS)
    along = jnp.mean(d_norm * rows_b, axis=-1, keepdims=True)
    d_input = d_norm * scale - rows_b * (scale * scale * scale * along)
    out_rows[0] = (grads_in[...].astype(F32) + d_input).astype(BF16)

    @pl.when(section > 0)
    def _():
        shift(0).start()

    out_rows[1] = (acts_in[...].astype(F32) + add_second(1)).astype(BF16)

    @pl.when(section < sections - 1)
    def _():
        shift(1).start()

    def pointwise_late(i, carry):
        at = pl.ds(pl.multiple_of(i * group, group), group)
        low = pl.ds(pl.multiple_of(tokens + i * group, group), group)
        dgate_out[at, :], dup_out[at, :] = back_of(acc_act[low, :], acc_gate[at, :], acc_up[at, :])
        return carry

    lax.fori_loop(0, tokens // group, pointwise_late, 0)

    @pl.when(section < sections - 1)
    def _():
        shift(0).wait_recv()
        next_grads[...] = in_rows[0]

    @pl.when(section == sections - 1)
    def _():
        next_grads[...] = jnp.zeros_like(next_grads)

    @pl.when(section > 0)
    def _():
        shift(1).wait_recv()
        next_acts[...] = in_rows[1]
        shift(0).wait_send()

    @pl.when(section == 0)
    def _():
        next_acts[...] = jnp.zeros_like(next_acts)

    @pl.when(section < sections - 1)
    def _():
        shift(1).wait_send()

    for r in range(2):
        core_copy(r).wait_send()
        first_copy(r).wait_send()
        second_copy(r).wait_send()
    for a in range(5):
        for slot in range(7):
            block_copy(a, own_b, slot, partner).wait_send()


def outer_kernel(late, d_gate, d_up, grad_gate, grad_up):
    right = late[...]
    grad_gate[...] = contract_rows(d_gate[...], right).astype(BF16)
    grad_up[...] = contract_rows(d_up[...], right).astype(BF16)


def outer(late, d_gate, d_up):
    tokens, width = late.shape
    hidden = d_gate.shape[1]
    whole = pl.BlockSpec((tokens, hidden), lambda i: (0, 0))
    tile = pl.BlockSpec((hidden, STEP), lambda i: (0, i))
    return pl.pallas_call(
        outer_kernel,
        grid=(width // STEP,),
        out_shape=(jax.ShapeDtypeStruct((hidden, width), BF16),) * 2,
        in_specs=[pl.BlockSpec((tokens, STEP), lambda i: (0, i)), whole, whole],
        out_specs=(tile, tile),
        cost_estimate=pl.CostEstimate(
            flops=4 * tokens * width * hidden, bytes_accessed=4 * width * hidden, transcendentals=0
        ),
    )(late, d_gate, d_up)


def body(weight_gate, weight_up, weight_down, acts_in, grads_in, saved_acts, saved_grads, plan):
    width, hidden = weight_gate.shape
    rows = acts_in.shape[1]
    blocks = 8
    tokens = rows * blocks
    vmem = pl.BlockSpec(memory_space=pltpu.VMEM)
    hbm = pl.BlockSpec(memory_space=pl.ANY)
    dma = pltpu.SemaphoreType.DMA
    small = jax.ShapeDtypeStruct((rows, width), BF16)
    narrow = jax.ShapeDtypeStruct((tokens, hidden), BF16)
    next_acts, next_grads, late, d_gate, d_up = pl.pallas_call(
        tick_kernel,
        out_shape=(small, small, jax.ShapeDtypeStruct((tokens, width), BF16), narrow, narrow),
        in_specs=[pl.BlockSpec(memory_space=pltpu.SMEM), hbm, hbm, hbm, vmem, vmem, vmem, vmem],
        out_specs=(vmem,) * 5,
        scratch_shapes=[
            pltpu.VMEM((hidden, width), BF16),
            pltpu.VMEM((hidden, width), BF16),
            pltpu.VMEM((hidden, width), BF16),
            pltpu.VMEM((5, blocks, rows, width), BF16),
            pltpu.VMEM((2 * tokens, width), BF16),
            pltpu.VMEM((2 * tokens, width), BF16),
            pltpu.VMEM((2 * tokens, hidden), F32),
            pltpu.VMEM((2 * tokens, hidden), F32),
            pltpu.VMEM((2 * tokens, hidden), F32),
            pltpu.VMEM((tokens, hidden), BF16),
            pltpu.VMEM((tokens, hidden), BF16),
            pltpu.VMEM((tokens, hidden), BF16),
            pltpu.VMEM((2, 2, 2, 2, rows, width), BF16),
            pltpu.VMEM((2, 2, 2, rows, width), BF16),
            pltpu.VMEM((2, 2, 2, rows, width), BF16),
            pltpu.VMEM((2, 2, rows, width), BF16),
            pltpu.VMEM((2, 2, rows, width), BF16),
            pltpu.VMEM((2, rows, width), BF16),
            pltpu.VMEM((2, rows, width), BF16),
            pltpu.VMEM((2, rows, width), BF16),
            dma((width // STEP,)),
            dma((width // STEP,)),
            dma((4,)),
            dma((5, 7)),
            dma((5, 7)),
            dma((2, 3)),
            dma((2, 3)),
            dma((2,)),
            dma((2,)),
        ],
        compiler_params=pltpu.CompilerParams(
            collective_id=0, has_side_effects=True, vmem_limit_bytes=64 * 1024 * 1000
        ),
    )(
        plan, weight_gate.T, weight_up.T, weight_down,
        acts_in[0], grads_in[0], saved_acts[0], saved_grads[0],
    )
    grad_gate, grad_up = outer(late, d_gate, d_up)
    return (next_acts[None], next_grads[None], grad_gate.T[None], grad_up.T[None])


def solution(mesh):
    placed = (
        P(None, ("dp", "tensor")),
        P(None, ("dp", "tensor")),
        P(("dp", "tensor"), None),
        P("section", ("dp", "tensor"), None),
        P("section", ("dp", "tensor"), None),
        P("section", None, ("dp", "tensor"), None),
        P("section", None, ("dp", "tensor"), None),
        P("section", None),
    )

    def chosen(*arrays):
        width = arrays[0].shape[0]
        rows = arrays[3].shape[1]
        square = mesh.shape["dp"] == 4 and mesh.shape["tensor"] == 2
        fits = square and rows % 8 == 0 and width % (2 * STEP) == 0 and arrays[0].shape[1] % 16 == 0
        return (body if fits else plain_body)(*arrays)

    return jax.shard_map(
        chosen,
        mesh=mesh,
        in_specs=placed,
        out_specs=(
            P("section", ("dp", "tensor"), None),
            P("section", ("dp", "tensor"), None),
            P("section", None, ("dp", "tensor")),
            P("section", None, ("dp", "tensor")),
        ),
        check_vma=False,
    )
```

```python
import jax
import jax.numpy as jnp
from jax import lax
from jax.experimental import pallas as pl
from jax.experimental.pallas import tpu as pltpu
from jax.sharding import PartitionSpec as P

EPS = 0.5


def shifted(block, axis, distance):
    devices = range(lax.axis_size(axis))
    route = [(i - distance, i) for i in devices if i - distance in devices]
    return lax.ppermute(block, axis, route)


def rms_scale(row_block):
    mean_sq = jnp.mean(row_block * row_block, axis=-1, keepdims=True)
    return row_block * lax.rsqrt(mean_sq + EPS)


def gated(normed, w_gate, w_up):
    gate_pre = jnp.dot(normed, w_gate, preferred_element_type=jnp.float32)
    up_pre = jnp.dot(normed, w_up, preferred_element_type=jnp.float32)
    return (gate_pre, up_pre)


def back_gates(cotangent, w_down, gate_pre, up_pre):
    d_act = lax.dot_general(
        cotangent, w_down, (((1,), (1,)), ((), ())), preferred_element_type=jnp.float32
    )
    sigmoid_gate = jax.nn.sigmoid(gate_pre)
    d_up = (d_act * gate_pre * sigmoid_gate).astype(jnp.bfloat16)
    d_gate = (d_act * up_pre * sigmoid_gate * (1.0 + gate_pre * (1.0 - sigmoid_gate))).astype(
        jnp.bfloat16
    )
    return (d_gate, d_up)


def contract_rows(left, right):
    return lax.dot_general(
        left, right, (((0,), (0,)), ((), ())), preferred_element_type=jnp.float32
    )


def plain_body(weight_gate, weight_up, weight_down, acts_in, grads_in, saved_acts, saved_grads, plan):
    front_rows = acts_in[0]
    cot_back = grads_in[0]
    back_rows = lax.dynamic_index_in_dim(saved_acts[0], plan[0, 0], 0, keepdims=False)
    late_rows = lax.dynamic_index_in_dim(saved_acts[0], plan[0, 1], 0, keepdims=False)
    cot_late = lax.dynamic_index_in_dim(saved_grads[0], plan[0, 1], 0, keepdims=False)
    norm_front = rms_scale(front_rows.astype(jnp.float32)).astype(jnp.bfloat16)
    norm_back = rms_scale(back_rows.astype(jnp.float32)).astype(jnp.bfloat16)
    norm_late = rms_scale(late_rows.astype(jnp.float32)).astype(jnp.bfloat16)
    in_group = (
        lax.all_gather(norm_front, "tensor", axis=0, tiled=True),
        lax.all_gather(norm_back, "tensor", axis=0, tiled=True),
        lax.all_gather(cot_back, "tensor", axis=0, tiled=True),
        lax.all_gather(norm_late, "tensor", axis=0, tiled=True),
        lax.all_gather(cot_late, "tensor", axis=0, tiled=True),
    )
    gathered = (
        lax.all_gather(in_group[0], "dp", axis=0, tiled=True),
        lax.all_gather(in_group[1], "dp", axis=0, tiled=True),
        lax.all_gather(in_group[2], "dp", axis=0, tiled=True),
        lax.all_gather(in_group[3], "dp", axis=0, tiled=True),
        lax.all_gather(in_group[4], "dp", axis=0, tiled=True),
    )
    all_front, all_back, all_cot_back, all_late, all_cot_late = gathered
    gate_front, up_front = gated(all_front, weight_gate, weight_up)
    act_front = (jax.nn.silu(gate_front) * up_front).astype(jnp.bfloat16)
    gate_back, up_back = gated(all_back, weight_gate, weight_up)
    dgate_back, dup_back = back_gates(all_cot_back, weight_down, gate_back, up_back)
    branch = jnp.dot(act_front, weight_down, preferred_element_type=jnp.float32)
    d_norm = lax.dot_general(
        dgate_back, weight_gate, (((1,), (1,)), ((), ())), preferred_element_type=jnp.float32
    )
    d_norm = d_norm + lax.dot_general(
        dup_back, weight_up, (((1,), (1,)), ((), ())), preferred_element_type=jnp.float32
    )
    dp_block = lax.psum_scatter(
        jnp.concatenate([branch, d_norm], axis=1).astype(jnp.bfloat16),
        "dp",
        scatter_dimension=0,
        tiled=True,
    )
    summed = lax.psum_scatter(dp_block, "tensor", scatter_dimension=0, tiled=True).astype(
        jnp.float32
    )
    model_width = front_rows.shape[1]
    branch_rows = summed[:, :model_width]
    d_norm_rows = summed[:, model_width:]
    out_front = (front_rows.astype(jnp.float32) + branch_rows).astype(jnp.bfloat16)
    unused, norm_pull = jax.vjp(rms_scale, back_rows.astype(jnp.float32))
    d_input = norm_pull(d_norm_rows)[0]
    d_rows = (cot_back.astype(jnp.float32) + d_input).astype(jnp.bfloat16)
    next_acts = shifted(out_front, "section", 1)
    next_grads = shifted(d_rows, "section", -1)
    gate_late, up_late = gated(all_late, weight_gate, weight_up)
    dgate_late, dup_late = back_gates(all_cot_late, weight_down, gate_late, up_late)
    grad_gate = contract_rows(all_late, dgate_late).astype(jnp.bfloat16)
    grad_up = contract_rows(all_late, dup_late).astype(jnp.bfloat16)
    return (next_acts[None], next_grads[None], grad_gate[None], grad_up[None])


STEP = 512
NT = (((1,), (1,)), ((), ()))
F32 = jnp.float32
BF16 = jnp.bfloat16
FRONT, BACK, COT_BACK, COT_LATE, LATE = range(5)


def tick_kernel(
    plan, w_gate, w_up, w_down, acts_in, grads_in, saved_acts, saved_grads,
    next_acts, next_grads, late_out, dgate_out, dup_out,
    gate_v, up_v, down_v, blocks, x_fb, x_gh, acc_gate, acc_up, acc_act, act_f, dgate_b, dup_b,
    part, recv_core, held, recv_first, held_next, recv_second, out_rows, in_rows,
    sem_gate, sem_up, sem_down, g_send, g_recv, r_send, r_recv, s_send, s_recv,
):
    dp, y, section = lax.axis_index("dp"), lax.axis_index("tensor"), lax.axis_index("section")
    sections = lax.axis_size("section")
    x, c = dp // 2, dp % 2
    rows, width = acts_in.shape
    steps = width // STEP
    down_cols = width // sem_down.shape[0]
    first_dp = ((1 - x) * (1 - c) + x * c) * 2 + c
    first_y = y * (1 - c) + (1 - y) * c
    second_dp = (x * (1 - c) + (1 - x) * c) * 2 + c
    second_y = (1 - y) * (1 - c) + y * c
    first = {"dp": first_dp, "tensor": first_y}
    second = {"dp": second_dp, "tensor": second_y}
    partner = {"dp": x * 2 + 1 - c}
    after = {"section": (section + 1) % sections}
    before = {"section": (section + sections - 1) % sections}
    own_b = dp * 2 + y
    first_b = first_dp * 2 + first_y
    second_b = second_dp * 2 + second_y
    far_b = ((1 - x) * 2 + c) * 2 + 1 - y
    other = 2 - 4 * c

    def gate_copy(k):
        at = pl.ds(pl.multiple_of(k * STEP, STEP), STEP)
        return pltpu.make_async_copy(w_gate.at[:, at], gate_v.at[:, at], sem_gate.at[k])

    def up_copy(k):
        at = pl.ds(pl.multiple_of(k * STEP, STEP), STEP)
        return pltpu.make_async_copy(w_up.at[:, at], up_v.at[:, at], sem_up.at[k])

    def down_copy(k):
        at = pl.ds(k * down_cols, down_cols)
        return pltpu.make_async_copy(w_down.at[:, at], down_v.at[:, at], sem_down.at[k])

    def start_weights(k, carry):
        gate_copy(k).start()
        up_copy(k).start()
        return carry

    lax.fori_loop(0, steps, start_weights, 0)
    for k in range(sem_down.shape[0]):
        down_copy(k).start()

    barrier = pltpu.get_barrier_semaphore()
    for peer in (first, second, partner, after, before):
        pl.semaphore_signal(barrier, inc=1, device_id=peer, device_id_type=pl.DeviceIdType.MESH)

    back_slot, late_slot = plan[0, 0], plan[0, 1]
    blocks[FRONT, own_b] = rms_scale(acts_in[...].astype(F32)).astype(BF16)
    blocks[BACK, own_b] = rms_scale(saved_acts[back_slot].astype(F32)).astype(BF16)
    blocks[COT_BACK, own_b] = grads_in[...]
    blocks[COT_LATE, own_b] = saved_grads[late_slot]
    blocks[LATE, own_b] = rms_scale(saved_acts[late_slot].astype(F32)).astype(BF16)
    pl.semaphore_wait(barrier, 5)

    def remote(src, dst, send, recv, peer):
        return pltpu.make_async_remote_copy(
            src_ref=src, dst_ref=dst, send_sem=send, recv_sem=recv,
            device_id=peer, device_id_type=pl.DeviceIdType.MESH,
        )

    def block_copy(a, b, slot, peer):
        return remote(blocks.at[a, b], blocks.at[a, b], g_send.at[a, slot], g_recv.at[a, slot], peer)

    def arrived(a, b, slot):
        block_copy(a, b, slot, partner).wait_recv()

    def send_own(a):
        block_copy(a, own_b, 0, first).start()
        block_copy(a, own_b, 1, second).start()
        block_copy(a, own_b, 3, partner).start()

    def relay(a):
        arrived(a, first_b, 0)
        block_copy(a, first_b, 2, second).start()
        block_copy(a, first_b, 4, partner).start()

    def finish(a):
        arrived(a, second_b, 1)
        block_copy(a, second_b, 5, partner).start()
        arrived(a, far_b, 2)
        block_copy(a, far_b, 6, partner).start()
        for slot, b in ((3, own_b), (4, second_b), (5, first_b), (6, far_b)):
            arrived(a, b + other, slot)

    def assemble(a, out, offset):
        def move(k, carry):
            at = pl.ds(pl.multiple_of(k * STEP, STEP), STEP)
            piece = blocks[a, :, :, at].astype(F32)
            out[offset : offset + piece.shape[0] * rows, at] = piece.reshape(-1, STEP).astype(BF16)
            return carry

        lax.fori_loop(0, steps, move, 0)

    tokens = blocks.shape[1] * rows
    send_own(FRONT)
    send_own(BACK)
    relay(FRONT)
    send_own(COT_BACK)
    relay(BACK)
    send_own(COT_LATE)
    finish(FRONT)
    assemble(FRONT, x_fb, 0)
    finish(BACK)
    assemble(BACK, x_fb, tokens)

    def up_front(k, carry):
        gate_copy(k).wait()
        up_copy(k).wait()
        at = pl.ds(pl.multiple_of(k * STEP, STEP), STEP)
        piece = x_fb[:, at]
        acc_gate[...] += lax.dot_general(piece, gate_v[:, at], NT, preferred_element_type=F32)
        acc_up[...] += lax.dot_general(piece, up_v[:, at], NT, preferred_element_type=F32)
        return carry

    acc_gate[...] = jnp.zeros_like(acc_gate)
    acc_up[...] = jnp.zeros_like(acc_up)
    lax.fori_loop(0, steps // 2, up_front, 0)
    relay(COT_BACK)
    send_own(LATE)
    relay(COT_LATE)
    lax.fori_loop(steps // 2, steps, up_front, 0)
    finish(COT_BACK)
    assemble(COT_BACK, x_gh, 0)
    relay(LATE)
    finish(COT_LATE)
    assemble(COT_LATE, x_gh, tokens)

    for k in range(sem_down.shape[0]):
        down_copy(k).wait()

    def d_act_step(k, carry):
        at = pl.ds(pl.multiple_of(k * STEP, STEP), STEP)
        acc_act[...] += lax.dot_general(x_gh[:, at], down_v[:, at], NT, preferred_element_type=F32)
        return carry

    acc_act[...] = jnp.zeros_like(acc_act)
    lax.fori_loop(0, steps, d_act_step, 0)

    def back_of(d_act, gate_pre, up_pre):
        sigmoid_gate = jax.nn.sigmoid(gate_pre)
        d_up = (d_act * gate_pre * sigmoid_gate).astype(BF16)
        d_gate = (d_act * up_pre * sigmoid_gate * (1.0 + gate_pre * (1.0 - sigmoid_gate))).astype(BF16)
        return d_gate, d_up

    group = 16

    def pointwise(i, carry):
        at = pl.ds(pl.multiple_of(i * group, group), group)
        low = pl.ds(pl.multiple_of(tokens + i * group, group), group)
        dgate_b[at, :], dup_b[at, :] = back_of(acc_act[at, :], acc_gate[low, :], acc_up[low, :])
        gate_pre = acc_gate[at, :]
        act_f[at, :] = (gate_pre * jax.nn.sigmoid(gate_pre) * acc_up[at, :]).astype(BF16)
        return carry

    lax.fori_loop(0, tokens // group, pointwise, 0)

    def put_part(r, at, total):
        for b in range(8):
            part[r, (b // 2) % 2, b // 4, b % 2, :, at] = total[b * rows : (b + 1) * rows].astype(BF16)

    def d_norm_step(k, carry):
        at = pl.ds(pl.multiple_of(k * STEP, STEP), STEP)
        total = jnp.dot(dgate_b[...], gate_v[:, at], preferred_element_type=F32)
        total += jnp.dot(dup_b[...], up_v[:, at], preferred_element_type=F32)
        put_part(0, at, total)
        return carry

    def branch_step(k, carry):
        at = pl.ds(pl.multiple_of(k * STEP, STEP), STEP)
        put_part(1, at, jnp.dot(act_f[...], down_v[:, at], preferred_element_type=F32))
        return carry

    mine_first = x * (1 - c) + y * c
    mine_second = y * (1 - c) + x * c

    def core_copy(r):
        return remote(part.at[r, 1 - c], recv_core.at[r], r_send.at[r, 0], r_recv.at[r, 0], partner)

    def first_copy(r):
        return remote(held.at[r, 1 - mine_first], recv_first.at[r], r_send.at[r, 1], r_recv.at[r, 1], first)

    def second_copy(r):
        return remote(held_next.at[r, 1 - mine_second], recv_second.at[r], r_send.at[r, 2], r_recv.at[r, 2], second)

    def add_core(r):
        core_copy(r).wait_recv()
        for f in range(2):
            for s in range(2):
                at_x = f * (1 - c) + s * c
                at_y = s * (1 - c) + f * c
                mine = part[r, c, at_x, at_y].astype(F32)
                held[r, f, s] = (mine + recv_core[r, at_x, at_y].astype(F32)).astype(BF16)
        first_copy(r).start()

    def add_first(r):
        first_copy(r).wait_recv()
        for s in range(2):
            mine = held[r, mine_first, s].astype(F32)
            held_next[r, s] = (mine + recv_first[r, s].astype(F32)).astype(BF16)
        second_copy(r).start()

    def add_second(r):
        second_copy(r).wait_recv()
        return held_next[r, mine_second].astype(F32) + recv_second[r].astype(F32)

    def shift(r):
        return remote(out_rows.at[r], in_rows.at[r], s_send.at[r], s_recv.at[r], before if r == 0 else after)

    lax.fori_loop(0, steps, d_norm_step, 0)
    core_copy(0).start()
    lax.fori_loop(0, steps, branch_step, 0)
    core_copy(1).start()
    add_core(0)
    finish(LATE)
    assemble(LATE, late_out, 0)

    def up_late(k, carry):
        at = pl.ds(pl.multiple_of(k * STEP, STEP), STEP)
        piece = late_out[:, at]
        acc_gate[:tokens] += lax.dot_general(piece, gate_v[:, at], NT, preferred_element_type=F32)
        acc_up[:tokens] += lax.dot_general(piece, up_v[:, at], NT, preferred_element_type=F32)
        return carry

    acc_gate[:tokens] = jnp.zeros((tokens, acc_gate.shape[1]), F32)
    acc_up[:tokens] = jnp.zeros((tokens, acc_up.shape[1]), F32)
    add_core(1)
    lax.fori_loop(0, steps // 2, up_late, 0)
    add_first(0)
    add_first(1)
    lax.fori_loop(steps // 2, steps, up_late, 0)

    d_norm = add_second(0)
    rows_b = saved_acts[back_slot].astype(F32)
    scale = lax.rsqrt(jnp.mean(rows_b * rows_b, axis=-1, keepdims=True) + EPS)
    along = jnp.mean(d_norm * rows_b, axis=-1, keepdims=True)
    d_input = d_norm * scale - rows_b * (scale * scale * scale * along)
    out_rows[0] = (grads_in[...].astype(F32) + d_input).astype(BF16)

    @pl.when(section > 0)
    def _():
        shift(0).start()

    out_rows[1] = (acts_in[...].astype(F32) + add_second(1)).astype(BF16)

    @pl.when(section < sections - 1)
    def _():
        shift(1).start()

    def pointwise_late(i, carry):
        at = pl.ds(pl.multiple_of(i * group, group), group)
        low = pl.ds(pl.multiple_of(tokens + i * group, group), group)
        dgate_out[at, :], dup_out[at, :] = back_of(acc_act[low, :], acc_gate[at, :], acc_up[at, :])
        return carry

    lax.fori_loop(0, tokens // group, pointwise_late, 0)

    @pl.when(section < sections - 1)
    def _():
        shift(0).wait_recv()
        next_grads[...] = in_rows[0]

    @pl.when(section == sections - 1)
    def _():
        next_grads[...] = jnp.zeros_like(next_grads)

    @pl.when(section > 0)
    def _():
        shift(1).wait_recv()
        next_acts[...] = in_rows[1]
        shift(0).wait_send()

    @pl.when(section == 0)
    def _():
        next_acts[...] = jnp.zeros_like(next_acts)

    @pl.when(section < sections - 1)
    def _():
        shift(1).wait_send()

    for r in range(2):
        core_copy(r).wait_send()
        first_copy(r).wait_send()
        second_copy(r).wait_send()
    for a in range(5):
        for slot in range(7):
            block_copy(a, own_b, slot, partner).wait_send()


def outer_kernel(late, d_gate, d_up, acts, grads, grad_gate, grad_up, next_acts, next_grads):
    next_acts[...] = acts[...]
    next_grads[...] = grads[...]
    right = late[...]
    grad_gate[...] = contract_rows(d_gate[...], right).astype(BF16)
    grad_up[...] = contract_rows(d_up[...], right).astype(BF16)


def outer(late, d_gate, d_up, acts, grads):
    tokens, width = late.shape
    hidden = d_gate.shape[1]
    whole = pl.BlockSpec((tokens, hidden), lambda i: (0, 0))
    slim = pl.BlockSpec((acts.shape[0], STEP), lambda i: (0, i))
    tile = pl.BlockSpec((hidden, STEP), lambda i: (0, i))
    return pl.pallas_call(
        outer_kernel,
        grid=(width // STEP,),
        out_shape=(jax.ShapeDtypeStruct((hidden, width), BF16),) * 2
        + (jax.ShapeDtypeStruct(acts.shape, BF16),) * 2,
        in_specs=[pl.BlockSpec((tokens, STEP), lambda i: (0, i)), whole, whole, slim, slim],
        out_specs=(tile, tile, slim, slim),
        cost_estimate=pl.CostEstimate(
            flops=4 * tokens * width * hidden, bytes_accessed=4 * width * hidden, transcendentals=0
        ),
    )(late, d_gate, d_up, acts, grads)


def body(weight_gate, weight_up, weight_down, acts_in, grads_in, saved_acts, saved_grads, plan):
    width, hidden = weight_gate.shape
    rows = acts_in.shape[1]
    blocks = 8
    tokens = rows * blocks
    vmem = pl.BlockSpec(memory_space=pltpu.VMEM)
    hbm = pl.BlockSpec(memory_space=pl.ANY)
    dma = pltpu.SemaphoreType.DMA
    small = jax.ShapeDtypeStruct((rows, width), BF16)
    narrow = jax.ShapeDtypeStruct((tokens, hidden), BF16)
    next_acts, next_grads, late, d_gate, d_up = pl.pallas_call(
        tick_kernel,
        out_shape=(small, small, jax.ShapeDtypeStruct((tokens, width), BF16), narrow, narrow),
        in_specs=[pl.BlockSpec(memory_space=pltpu.SMEM), hbm, hbm, hbm, vmem, vmem, vmem, vmem],
        out_specs=(vmem,) * 5,
        scratch_shapes=[
            pltpu.VMEM((hidden, width), BF16),
            pltpu.VMEM((hidden, width), BF16),
            pltpu.VMEM((hidden, width), BF16),
            pltpu.VMEM((5, blocks, rows, width), BF16),
            pltpu.VMEM((2 * tokens, width), BF16),
            pltpu.VMEM((2 * tokens, width), BF16),
            pltpu.VMEM((2 * tokens, hidden), F32),
            pltpu.VMEM((2 * tokens, hidden), F32),
            pltpu.VMEM((2 * tokens, hidden), F32),
            pltpu.VMEM((tokens, hidden), BF16),
            pltpu.VMEM((tokens, hidden), BF16),
            pltpu.VMEM((tokens, hidden), BF16),
            pltpu.VMEM((2, 2, 2, 2, rows, width), BF16),
            pltpu.VMEM((2, 2, 2, rows, width), BF16),
            pltpu.VMEM((2, 2, 2, rows, width), BF16),
            pltpu.VMEM((2, 2, rows, width), BF16),
            pltpu.VMEM((2, 2, rows, width), BF16),
            pltpu.VMEM((2, rows, width), BF16),
            pltpu.VMEM((2, rows, width), BF16),
            pltpu.VMEM((2, rows, width), BF16),
            dma((width // STEP,)),
            dma((width // STEP,)),
            dma((4,)),
            dma((5, 7)),
            dma((5, 7)),
            dma((2, 3)),
            dma((2, 3)),
            dma((2,)),
            dma((2,)),
        ],
        compiler_params=pltpu.CompilerParams(
            collective_id=0, has_side_effects=True, vmem_limit_bytes=64 * 1024 * 1000
        ),
    )(
        plan, weight_gate.T, weight_up.T, weight_down,
        acts_in[0], grads_in[0], saved_acts[0], saved_grads[0],
    )
    grad_gate, grad_up, next_acts, next_grads = outer(late, d_gate, d_up, next_acts, next_grads)
    return (next_acts[None], next_grads[None], grad_gate.T[None], grad_up.T[None])


def solution(mesh):
    placed = (
        P(None, ("dp", "tensor")),
        P(None, ("dp", "tensor")),
        P(("dp", "tensor"), None),
        P("section", ("dp", "tensor"), None),
        P("section", ("dp", "tensor"), None),
        P("section", None, ("dp", "tensor"), None),
        P("section", None, ("dp", "tensor"), None),
        P("section", None),
    )

    def chosen(*arrays):
        width = arrays[0].shape[0]
        rows = arrays[3].shape[1]
        square = mesh.shape["dp"] == 4 and mesh.shape["tensor"] == 2
        fits = square and rows % 8 == 0 and width % (2 * STEP) == 0 and arrays[0].shape[1] % 16 == 0
        return (body if fits else plain_body)(*arrays)

    return jax.shard_map(
        chosen,
        mesh=mesh,
        in_specs=placed,
        out_specs=(
            P("section", ("dp", "tensor"), None),
            P("section", ("dp", "tensor"), None),
            P("section", None, ("dp", "tensor")),
            P("section", None, ("dp", "tensor")),
        ),
        check_vma=False,
    )
```
